32 devices in a mesh: dp: 8 (over y, x, core), mp: 4 (over z).
Axes of the slice: x: 2, y: 2, z: 4, core: 2. Of those that a mesh axis runs over, the one named last changes fastest.
Arguments:
- states: bfloat16 [128, 80, 768], P('dp'), may hold values from -6 to 6
- hist_len: int32 [128], P('dp'), may hold values from 1 to 20
- norm_gain: float32 [768], replicated, may hold values from 0.5 to 1.5
- qkv_weight: bfloat16 [768, 3, 12, 64], P(None, None, 'mp'), may hold values from -1 to 1
- output_weight: bfloat16 [12, 64, 768], P('mp'), may hold values from -0.21875 to 0.21875
- cotangent: bfloat16 [128, 80, 768], P('dp'), may hold values from -6 to 6
Outputs:
- attended: bfloat16 [128, 80, 768], P('dp')
- grad_states: bfloat16 [128, 80, 768], P('dp')
- grad_qkv: float32 [768, 3, 12, 64], P('dp', None, 'mp')
- output_weight_gradient: float32 [12, 64, 768], P('mp', None, 'dp')
- grad_gain: float32 [768], P('dp')
The draws below stay inside these ranges and needn't reach their ends.
All inputs are finite; a program needn't handle non-finite values.
Results may differ from the reference program's by a relative error of at most 0.012.
Values may be sent and summed in bfloat16 or wider, within the bound.
A program may use at most 128 MiB of HBM per device.

```python
import jax
import jax.numpy as jnp
from jax import lax

D = 768
H = 12
DH = 64
ITEMS = 20
LEVELS = 4
S = 80
B = 128


def draw_qkv_weight(key, part):
    k_base, k_noise, k_value = jax.random.split(key, 3)
    inverse = D ** (-0.5)
    query_part = 0.5 * inverse * jax.random.normal(k_base, (D, H, DH), jnp.float32)
    key_part = 0.5 * inverse * jax.random.normal(k_noise, (D, H, DH), jnp.float32)
    value_part = inverse * jax.random.normal(k_value, (D, H, DH), jnp.float32)
    stacked = jnp.stack([query_part, key_part, value_part], axis=1)
    return jnp.clip(stacked, -1.0, 1.0).astype(jnp.bfloat16)


def set_ends(drawn, own_key, least, high):
    longest = drawn.shape.index(max(drawn.shape))
    spots = []
    for shift in (0, 1):
        where = [jax.random.randint(jax.random.fold_in(own_key, axis), (), 0, length) for axis, length in enumerate(drawn.shape)]
        where[longest] = (where[longest] + shift) % drawn.shape[longest]
        spots.append(tuple(where))
    return drawn.at[spots[0]].set(least).at[spots[1]].set(high)


def with_spikes(drawn, key, source, target, blocks, factor):
    def block_of(dim):
        return (jnp.arange(drawn.shape[dim]) // (drawn.shape[dim] // blocks)).reshape((-1,) + (1,) * (drawn.ndim - 1 - dim))

    first = jax.random.permutation(key, blocks)[block_of(target)]
    far = (block_of(target) + blocks // 2) % blocks
    return jnp.where((block_of(source) == first) | (block_of(source) == far), factor * drawn, drawn)


def block_levels(stream_key, extent, cuts, smallest, high):
    level, own = 1.0, jax.random.fold_in(stream_key, 6)
    for dim, blocks in cuts:
        heights = jnp.exp(jax.random.uniform(jax.random.fold_in(own, dim), (blocks,), jnp.float32, smallest / len(cuts), high / len(cuts)))
        level = level * jnp.repeat(heights, extent[dim] // blocks).reshape([-1 if axis == dim else 1 for axis in range(len(extent))])
    return level


def gaussian(own_key, shape, deviation, limit, pieces=(), kind=jnp.bfloat16):
    array = jax.random.normal(own_key, shape, jnp.float32) * deviation
    if len(pieces) > 0:
        array = block_levels(own_key, shape, pieces, -0.22, 0.18) * array
    return jnp.clip(array, min=-limit, max=limit).astype(kind)


def gaussian_with(rng, shape, deviation, reach, cuts, heavy, kind=jnp.bfloat16):
    result = deviation * jax.random.normal(rng, shape, jnp.float32)
    if cuts:
        result = result * block_levels(rng, shape, cuts, -0.22, 0.18)
    return jnp.clip(with_spikes(result, jax.random.fold_in(rng, 3), *heavy), -reach, reach).astype(kind)


def setup_inputs(seed: int = 0) -> dict:
    keys = jax.random.split(jax.random.key(seed), 7)
    states = gaussian_with(keys[0], (B, S, D), 1.0, 6.0, ((0, 8),), (0, 2, 8, 2.0))
    hist_len = set_ends(jax.random.randint(keys[1], (B,), 1, ITEMS + 1), jax.random.fold_in(keys[1], 1), 1, ITEMS).astype(jnp.int32)
    norm_gain = jnp.clip(1.0 + 0.1 * jax.random.normal(keys[2], (D,), jnp.float32), 0.5, 1.5)
    qkv_weight = draw_qkv_weight(jax.random.fold_in(keys[6], 71), 0)
    output_weight = gaussian(keys[4], (H, DH, D), (H * DH) ** -0.5, 0.21875, ((0, 4),))
    cotangent = gaussian_with(keys[5], (B, S, D), 1.0, 6.0, ((0, 8),), (0, 2, 8, 2.0))
    return {"states": states, "hist_len": hist_len, "norm_gain": norm_gain, "qkv_weight": qkv_weight, "output_weight": output_weight, "cotangent": cotangent}


def reference(states, hist_len, norm_gain, qkv_weight, output_weight, cotangent):
    wide_states = states.astype(jnp.float32)
    inv_rms = lax.rsqrt(lax.optimization_barrier(jnp.mean(wide_states * wide_states, axis=-1, keepdims=True)) + 1e-06)
    unit = wide_states * inv_rms
    normed = (unit * norm_gain).astype(jnp.bfloat16)
    proj = jnp.einsum('bsd,dchk->bschk', normed.astype(jnp.float32), qkv_weight.astype(jnp.float32)).astype(jnp.bfloat16)
    queries = proj[:, :, 0].astype(jnp.float32)
    key_rows = proj[:, :, 1].astype(jnp.float32)
    value_rows = proj[:, :, 2].astype(jnp.float32)
    positions = jnp.arange(states.shape[1], dtype=jnp.int32)
    keep_mask = positions[None, :] < LEVELS * hist_len[:, None]
    scores = jnp.einsum('bqhk,bphk->bhqp', queries, key_rows)
    masked = jnp.where(keep_mask[:, None, None, :], scores, -1e+30)
    row_top = lax.optimization_barrier(jnp.max(masked, axis=-1, keepdims=True))
    exp_scores = jnp.exp(masked - row_top)
    attn_prob = exp_scores / lax.optimization_barrier(jnp.sum(exp_scores, axis=-1, keepdims=True))
    prob_bf = attn_prob.astype(jnp.bfloat16).astype(jnp.float32)
    attended_context = jnp.einsum('bhqp,bphk->bqhk', prob_bf, value_rows).astype(jnp.bfloat16)
    mixed_total_sum = jnp.einsum('zagm,gms->zas', attended_context.astype(jnp.float32), output_weight.astype(jnp.float32))
    attended = (wide_states + mixed_total_sum).astype(jnp.bfloat16)
    masked_cotangent = jnp.where(keep_mask[:, :, None], cotangent, jnp.zeros_like(cotangent)).astype(jnp.float32)
    output_weight_gradient = jnp.einsum('wmep,wmx->epx', attended_context.astype(jnp.float32), masked_cotangent)
    context_gradient = jnp.einsum('uxy,wgy->uxwg', masked_cotangent, output_weight.astype(jnp.float32)).astype(jnp.bfloat16).astype(jnp.float32)
    grad_prob = jnp.einsum('bqhk,bphk->bhqp', context_gradient, value_rows)
    row_delta = lax.optimization_barrier(jnp.sum(attn_prob * grad_prob, axis=-1, keepdims=True))
    grad_score = (attn_prob * (grad_prob - row_delta)).astype(jnp.bfloat16).astype(jnp.float32)
    grad_query = jnp.einsum('bhqp,bphk->bqhk', grad_score, key_rows)
    grad_key = jnp.einsum('bhqp,bqhk->bphk', grad_score, queries)
    grad_value = jnp.einsum('bhqp,bqhk->bphk', prob_bf, context_gradient)
    grad_proj = jnp.stack([grad_query, grad_key, grad_value], axis=2).astype(jnp.bfloat16).astype(jnp.float32)
    grad_qkv = jnp.einsum('bsd,bschk->dchk', normed.astype(jnp.float32), grad_proj)
    grad_normed = jnp.einsum('bschk,dchk->bsd', grad_proj, qkv_weight.astype(jnp.float32))
    grad_gain = lax.optimization_barrier(jnp.sum(grad_normed * unit, axis=(0, 1)))
    grad_unit = grad_normed * norm_gain
    row_corr = lax.optimization_barrier(jnp.mean(grad_unit * unit, axis=-1, keepdims=True))
    grad_states = (masked_cotangent + inv_rms * (grad_unit - unit * row_corr)).astype(jnp.bfloat16)
    return (attended, grad_states, grad_qkv, output_weight_gradient, grad_gain)
```

```python
import functools

import jax
import jax.numpy as jnp
from jax import lax
from jax.experimental import pallas as pl
from jax.experimental.pallas import tpu as pltpu
from jax.sharding import PartitionSpec as P

LEVELS = 4
PIECES = 8
GROUP = 4
BF = jnp.bfloat16
F32 = jnp.float32
MESH = pl.DeviceIdType.MESH


def dot(a, b, ca, cb):
    return lax.dot_general(a, b, (((ca,), (cb,)), ((), ())), preferred_element_type=F32)


def remote(src, dst, ssem, rsem, device):
    return pltpu.make_async_remote_copy(
        src_ref=src, dst_ref=dst, send_sem=ssem, recv_sem=rsem, device_id=device, device_id_type=MESH
    )


def gather_kernel(n, own, wall, s_z, r_z, s_xy, r_xy, s_c, r_c):
    d, z = lax.axis_index("dp"), lax.axis_index("mp")
    c, bx, by = d % 2, (d // 2) % 2, (d // 4) % 2
    par = (bx + by) % 2
    partner = (d + 1 - 2 * c, z)
    across = ((d + 2 - 4 * bx, z), (d + 4 - 8 * by, z))
    barrier = pltpu.get_barrier_semaphore()
    greet = [(d, (z + n - j) % n) for j in range(1, n)] + list(across) + [partner]
    for device in greet:
        pl.semaphore_signal(barrier, inc=1, device_id=device, device_id_type=MESH)
    pl.semaphore_wait(barrier, len(greet))

    mine = [4 * par + 2 * i + c for i in range(2)]
    theirs = [4 * (1 - par) + 2 * i + c for i in range(2)]
    far = [4 * par + 2 * i + 1 - c for i in range(2)] + [4 * (1 - par) + 2 * i + 1 - c for i in range(2)]
    order = [j for j in (1, n - 1) if j < n] + [j for j in range(2, n - 1)]
    sends = []

    def go(src, dst, ssem, rsem, device):
        copy = remote(src, dst, ssem, rsem, device)
        copy.start()
        sends.append(copy)

    for j in order:
        for i in range(2):
            go(own.at[mine[i]], wall.at[j - 1, mine[i]], s_z.at[i, j - 1], r_z.at[i, j - 1], (d, (z + n - j) % n))
    for j in order:
        for i in range(2):
            spot = wall.at[j - 1, mine[i]]
            remote(spot, spot, s_z.at[i, j - 1], r_z.at[i, j - 1], partner).wait_recv()
            go(spot, spot, s_xy.at[i, j - 1], r_xy.at[i, j - 1], across[i])
            go(spot, spot, s_c.at[i, j - 1], r_c.at[i, j - 1], partner)
    for j in order:
        for i in range(2):
            spot = wall.at[j - 1, theirs[i]]
            remote(spot, spot, s_xy.at[i, j - 1], r_xy.at[i, j - 1], partner).wait_recv()
            go(spot, spot, s_c.at[2 + i, j - 1], r_c.at[2 + i, j - 1], partner)
    for j in order:
        for i in range(4):
            spot = wall.at[j - 1, far[i]]
            remote(spot, spot, s_c.at[i, j - 1], r_c.at[i, j - 1], partner).wait_recv()
    for copy in sends:
        copy.wait_send()


def gather(own, n):
    pairs = pltpu.SemaphoreType.DMA((2, n - 1))
    quads = pltpu.SemaphoreType.DMA((4, n - 1))
    return pl.pallas_call(
        functools.partial(gather_kernel, n),
        out_shape=jax.ShapeDtypeStruct((n - 1,) + own.shape, own.dtype),
        in_specs=[pl.BlockSpec(memory_space=pl.ANY)],
        out_specs=pl.BlockSpec(memory_space=pl.ANY),
        scratch_shapes=[pairs, pairs, pairs, pairs, quads, quads],
        compiler_params=pltpu.CompilerParams(collective_id=1, has_side_effects=True),
        name="gather",
    )(own)


def scatter_kernel(half, part, out, got, total, held, s_c, r_c, s_o, r_o):
    d, z = lax.axis_index("dp"), lax.axis_index("mp")
    c, chip = d % 2, d // 2
    partner = (d + 1 - 2 * c, z)
    others = [(((chip + o) % half) * 2 + c, z) for o in range(1, half)]
    barrier = pltpu.get_barrier_semaphore()
    for device in others + [partner]:
        pl.semaphore_signal(barrier, inc=1, device_id=device, device_id_type=MESH)
    pl.semaphore_wait(barrier, half)
    order = list(range(1, half)) + [0]
    sends = []
    for o in order:
        t = (chip + o) % half
        copy = remote(part.at[1 - c, t], got.at[o], s_c.at[o], r_c.at[o], partner)
        copy.start()
        sends.append(copy)
    for o in order:
        t = (chip + o) % half
        remote(got.at[o], got.at[o], s_c.at[o], r_c.at[o], partner).wait_recv()
        both = part[c, t].astype(F32) + got[o].astype(F32)
        if o == 0:
            out[...] = both
        else:
            total[o - 1] = both.astype(BF)
            copy = remote(total.at[o - 1], held.at[o - 1], s_o.at[o - 1], r_o.at[o - 1], others[o - 1])
            copy.start()
            sends.append(copy)
    for o in range(1, half):
        remote(held.at[o - 1], held.at[o - 1], s_o.at[o - 1], r_o.at[o - 1], partner).wait_recv()
        out[...] += held[o - 1].astype(F32)
    for copy in sends:
        copy.wait_send()


def scatter(part):
    _, half, rows, wide = part.shape
    return pl.pallas_call(
        functools.partial(scatter_kernel, half),
        out_shape=jax.ShapeDtypeStruct((rows, wide), F32),
        in_specs=[pl.BlockSpec(memory_space=pltpu.VMEM)],
        out_specs=pl.BlockSpec(memory_space=pltpu.VMEM),
        scratch_shapes=[
            pltpu.VMEM((half, rows, wide), BF),
            pltpu.VMEM((half - 1, rows, wide), BF),
            pltpu.VMEM((half - 1, rows, wide), BF),
            pltpu.SemaphoreType.DMA((half,)),
            pltpu.SemaphoreType.DMA((half,)),
            pltpu.SemaphoreType.DMA((half - 1,)),
            pltpu.SemaphoreType.DMA((half - 1,)),
        ],
        compiler_params=pltpu.CompilerParams(collective_id=2, has_side_effects=True),
        name="scatter",
    )(part)


def work_kernel(nb, n, width, hist, states, cot, gain, own, wall, att, gst, part,
                wq, wo, acc, gacc, proj, gproj, ctx, gctx, sems):
    i = pl.program_id(0)
    _, s, dim = states.shape
    rows = nb * s
    lanes = GROUP * 64

    @pl.when(i == 0)
    def _():
        copies = []
        for j in range(n):
            src = own if j == 0 else wall.at[j - 1]
            for k in range(4):
                at = pl.ds(k * width, width)
                dst = wo.at[pl.ds(j * width, width)] if k == 3 else wq.at[pl.ds(k * n * width + j * width, width)]
                copies.append(pltpu.make_async_copy(src.at[at], dst, sems.at[j, k]))
        for copy in copies:
            copy.start()
        acc[...] = jnp.zeros_like(acc)
        gacc[...] = jnp.zeros_like(gacc)
        for copy in copies:
            copy.wait()

    wide = states[...].reshape(rows, dim).astype(F32)
    inv = lax.rsqrt(jnp.mean(wide * wide, axis=-1, keepdims=True) + 1e-06)
    unit = wide * inv
    normed = (unit * gain[...]).astype(BF)
    for k in range(3):
        cols = pl.ds(k * dim, dim)
        proj[:, cols] = dot(normed, wq[cols, :], 1, 1).astype(BF)
    pos = lax.broadcasted_iota(jnp.int32, (s, dim), 0)
    mcot = jnp.concatenate(
        [jnp.where(pos < LEVELS * hist[i * nb + b], cot[b].astype(F32), 0.0) for b in range(nb)], axis=0
    ).astype(BF)
    gctx[...] = dot(mcot, wo[...], 1, 1).astype(BF)

    lane = lax.broadcasted_iota(jnp.int32, (s, lanes), 1) // 64
    key_pos = lax.broadcasted_iota(jnp.int32, (GROUP, s, s), 1)

    def spread(x):
        x = x.astype(F32)
        return jnp.concatenate([jnp.where(lane == h, x, 0.0).astype(BF) for h in range(GROUP)], axis=0)

    def fold(x):
        out = x[(GROUP - 1) * s :]
        for h in range(GROUP - 1):
            out = jnp.where(lane == h, x[h * s : (h + 1) * s], out)
        return out.astype(BF)

    @pl.loop(0, nb)
    def _(b):
        at = pl.ds(pl.multiple_of(b * s, 16), s)
        keep = key_pos < LEVELS * hist[i * nb + b]
        for g in range(dim // lanes):
            cols = [pl.ds(k * dim + g * lanes, lanes) for k in range(3)]
            here = pl.ds(g * lanes, lanes)
            q, gc = proj[at, cols[0]], gctx[at, here]
            kk, vv = spread(proj[at, cols[1]]), spread(proj[at, cols[2]])
            sc = dot(kk, q, 1, 1).reshape(GROUP, s, s)
            sc = jnp.where(keep, sc, -1e30)
            ex = jnp.exp(sc - jnp.max(sc, axis=1, keepdims=True))
            prob = ex * (1.0 / jnp.sum(ex, axis=1, keepdims=True))
            pb = prob.reshape(GROUP * s, s).astype(BF)
            ctx[at, here] = dot(pb, vv, 0, 0).astype(BF)
            gp = dot(vv, gc, 1, 1).reshape(GROUP, s, s)
            delta = jnp.sum(prob * gp, axis=1, keepdims=True)
            ds = (prob * (gp - delta)).reshape(GROUP * s, s).astype(BF)
            gproj[at, cols[0]] = dot(ds, kk, 0, 0).astype(BF)
            gproj[at, cols[1]] = fold(dot(ds, q, 1, 0))
            gproj[at, cols[2]] = fold(dot(pb, gc, 1, 0))

    att[...] = (wide + dot(ctx[...], wo[...], 1, 0)).astype(BF).reshape(nb, s, dim)
    gn = dot(gproj[...], wq[...], 1, 0)
    for k in range(3):
        acc[:, k * lanes : (k + 1) * lanes] += dot(normed, gproj[:, k * dim : k * dim + lanes], 0, 0)
    acc[:, 3 * lanes :] += dot(mcot, ctx[:, :lanes], 0, 0)
    gacc[...] += jnp.sum((gn * unit).reshape(rows // 8, 8, dim), axis=0)
    gu = gn * gain[...]
    corr = jnp.mean(gu * unit, axis=-1, keepdims=True)
    gst[...] = (mcot.astype(F32) + inv * (gu - unit * corr)).astype(BF).reshape(nb, s, dim)

    @pl.when(i == pl.num_programs(0) - 1)
    def _():
        total = jnp.sum(gacc[...], axis=0, keepdims=True)
        column = jnp.broadcast_to(total, (128, dim)).T
        high = column.astype(BF).astype(F32)
        at = lax.broadcasted_iota(jnp.int32, (dim, 128), 1)
        last = slice(4 * lanes - 128, 4 * lanes)
        acc[:, last] = jnp.where(at < 64, acc[:, last], jnp.where(at < 96, high, column - high))
        _, half, piece, _ = part.shape
        for t in range(2 * half):
            part[t % 2, t // 2] = acc[t * piece : (t + 1) * piece, :].astype(BF)


def work(states, hist, gain, own, wall, cot, n, nd):
    count, s, dim = states.shape
    nb = 4 if count % 4 == 0 else 1
    rows, lanes = nb * s, GROUP * 64
    width = dim // n
    block = pl.BlockSpec((nb, s, dim), lambda i, *_: (i, 0, 0))
    piece = (2, nd // 2, dim // nd, 4 * lanes)
    return pl.pallas_call(
        functools.partial(work_kernel, nb, n, width),
        out_shape=(
            jax.ShapeDtypeStruct(states.shape, BF),
            jax.ShapeDtypeStruct(states.shape, BF),
            jax.ShapeDtypeStruct(piece, BF),
        ),
        grid_spec=pltpu.PrefetchScalarGridSpec(
            num_scalar_prefetch=1,
            grid=(count // nb,),
            in_specs=[
                block,
                block,
                pl.BlockSpec((1, dim), lambda i, *_: (0, 0)),
                pl.BlockSpec(memory_space=pl.ANY),
                pl.BlockSpec(memory_space=pl.ANY),
            ],
            out_specs=[block, block, pl.BlockSpec(piece, lambda i, *_: (0, 0, 0, 0))],
            scratch_shapes=[
                pltpu.VMEM((3 * dim, dim), BF),
                pltpu.VMEM((dim, dim), BF),
                pltpu.VMEM((dim, 4 * lanes), F32),
                pltpu.VMEM((8, dim), F32),
                pltpu.VMEM((rows, 3 * dim), BF),
                pltpu.VMEM((rows, 3 * dim), BF),
                pltpu.VMEM((rows, dim), BF),
                pltpu.VMEM((rows, dim), BF),
                pltpu.SemaphoreType.DMA((n, 4)),
            ],
        ),
        compiler_params=pltpu.CompilerParams(
            dimension_semantics=("arbitrary",), vmem_limit_bytes=56 * 1024 * 1024
        ),
        name="work",
    )(hist, states, cot, gain.reshape(1, dim), own, wall)


def body(nd, n, states, hist_len, norm_gain, qkv_weight, output_weight, cotangent):
    dim, _, heads, size = qkv_weight.shape
    width = heads * size
    lanes = GROUP * 64
    own = jnp.concatenate([qkv_weight.reshape(dim, 3 * width).T, output_weight.reshape(width, dim)], axis=0)
    wall = gather(own.reshape(PIECES, 4 * width // PIECES, dim), n).reshape(n - 1, 4 * width, dim)
    attended, grad_states, part = work(states, hist_len, norm_gain, own, wall, cotangent, n, nd)
    summed = scatter(part)
    grads = summed.reshape(dim // nd, 4, lanes)
    grad_qkv = grads[:, :3, :width].reshape(dim // nd, 3, heads, size)
    grad_out = grads[:, 3, :width].T.reshape(heads, size, dim // nd)
    grad_gain = grads[:, 3, 192] + grads[:, 3, 224]
    return attended, grad_states, grad_qkv, grad_out, grad_gain


def solution(mesh):
    placed = (
        P("dp", None, None),
        P("dp"),
        P(),
        P(None, None, "mp", None),
        P("mp", None, None),
        P("dp", None, None),
    )
    return jax.shard_map(
        functools.partial(body, mesh.shape["dp"], mesh.shape["mp"]),
        mesh=mesh,
        in_specs=placed,
        out_specs=(
            P("dp", None, None),
            P("dp", None, None),
            P("dp", None, "mp", None),
            P("mp", None, "dp"),
            P("dp"),
        ),
        check_vma=False,
    )
```

```python
import functools

import jax
import jax.numpy as jnp
from jax import lax
from jax.experimental import pallas as pl
from jax.experimental.pallas import tpu as pltpu
from jax.sharding import PartitionSpec as P

LEVELS = 4
PIECES = 16
GROUP = 4
PACK = 2
BF = jnp.bfloat16
F32 = jnp.float32
MESH = pl.DeviceIdType.MESH


def dot(a, b, ca, cb):
    return lax.dot_general(a, b, (((ca,), (cb,)), ((), ())), preferred_element_type=F32)


def remote(src, dst, ssem, rsem, device):
    return pltpu.make_async_remote_copy(
        src_ref=src, dst_ref=dst, send_sem=ssem, recv_sem=rsem, device_id=device, device_id_type=MESH
    )


def gather_kernel(n, own, wall, s_z, r_z, s_x, r_x, s_d, r_d, s_c, r_c):
    d, z = lax.axis_index("dp"), lax.axis_index("mp")
    c, bx, by = d % 2, (d // 2) % 2, (d // 4) % 2
    partner = (d + 1 - 2 * c, z)
    across = ((d + 2 - 4 * bx, z), (d + 4 - 8 * by, z))
    barrier = pltpu.get_barrier_semaphore()
    greet = [(d, (z + n - j) % n) for j in range(1, n)] + list(across) + [partner]
    for device in greet:
        pl.semaphore_signal(barrier, inc=1, device_id=device, device_id_type=MESH)
    pl.semaphore_wait(barrier, len(greet))

    def place(x, y, core):
        return 4 * (x + 2 * y) + 2 * core

    mine = place(bx, by, c)
    sides = (place(1 - bx, by, c), place(bx, 1 - by, c))
    diag = place(1 - bx, 1 - by, c)
    order = [j for j in (1, n - 1) if j < n] + [j for j in range(2, n - 1)]
    sends = []

    def go(src, dst, ssem, rsem, device):
        copy = remote(src, dst, ssem, rsem, device)
        copy.start()
        sends.append(copy)

    def arrived(spot, rsem):
        remote(spot, spot, rsem, rsem, partner).wait_recv()

    for j in order:
        go(own.at[pl.ds(mine, 2)], wall.at[j - 1, pl.ds(mine, 2)], s_z.at[j - 1], r_z.at[j - 1], (d, (z + n - j) % n))
    for j in order:
        spot = wall.at[j - 1, pl.ds(mine, 2)]
        arrived(spot, r_z.at[j - 1])
        for i in range(2):
            go(spot, spot, s_x.at[i, j - 1], r_x.at[i, j - 1], across[i])
        go(spot, spot, s_c.at[0, j - 1], r_c.at[0, j - 1], partner)
    for j in order:
        for i in range(2):
            spot = wall.at[j - 1, pl.ds(sides[i], 2)]
            arrived(spot, r_x.at[i, j - 1])
            piece = wall.at[j - 1, sides[i] + i]
            go(piece, piece, s_d.at[i, j - 1], r_d.at[i, j - 1], across[1 - i])
            go(spot, spot, s_c.at[1 + i, j - 1], r_c.at[1 + i, j - 1], partner)
    for j in order:
        for i in range(2):
            piece = wall.at[j - 1, diag + i]
            arrived(piece, r_d.at[i, j - 1])
            go(piece, piece, s_c.at[3 + i, j - 1], r_c.at[3 + i, j - 1], partner)
    flip = 2 - 4 * c
    for j in order:
        for k, spot in enumerate((mine, sides[0], sides[1])):
            arrived(wall.at[j - 1, pl.ds(spot + flip, 2)], r_c.at[k, j - 1])
        for i in range(2):
            arrived(wall.at[j - 1, diag + i + flip], r_c.at[3 + i, j - 1])
    for copy in sends:
        copy.wait_send()


def gather(own, n):
    one, two, five = (pltpu.SemaphoreType.DMA(k + (n - 1,)) for k in ((), (2,), (5,)))
    return pl.pallas_call(
        functools.partial(gather_kernel, n),
        out_shape=jax.ShapeDtypeStruct((n - 1,) + own.shape, own.dtype),
        in_specs=[pl.BlockSpec(memory_space=pl.ANY)],
        out_specs=pl.BlockSpec(memory_space=pl.ANY),
        scratch_shapes=[one, one, two, two, two, two, five, five],
        compiler_params=pltpu.CompilerParams(collective_id=1, has_side_effects=True),
        name="gather",
    )(own)


def scatter_kernel(half, part, out, got, total, held, s_c, r_c, s_o, r_o):
    d, z = lax.axis_index("dp"), lax.axis_index("mp")
    c, chip = d % 2, d // 2
    partner = (d + 1 - 2 * c, z)
    others = [(((chip + o) % half) * 2 + c, z) for o in range(1, half)]
    barrier = pltpu.get_barrier_semaphore()
    for device in others + [partner]:
        pl.semaphore_signal(barrier, inc=1, device_id=device, device_id_type=MESH)
    pl.semaphore_wait(barrier, half)
    order = list(range(1, half)) + [0]
    sends = []
    for o in order:
        t = (chip + o) % half
        copy = remote(part.at[1 - c, t], got.at[o], s_c.at[o], r_c.at[o], partner)
        copy.start()
        sends.append(copy)
    for o in order:
        t = (chip + o) % half
        remote(got.at[o], got.at[o], s_c.at[o], r_c.at[o], partner).wait_recv()
        both = part[c, t].astype(F32) + got[o].astype(F32)
        if o == 0:
            out[...] = both
        else:
            total[o - 1] = both.astype(BF)
            copy = remote(total.at[o - 1], held.at[o - 1], s_o.at[o - 1], r_o.at[o - 1], others[o - 1])
            copy.start()
            sends.append(copy)
    for o in range(1, half):
        remote(held.at[o - 1], held.at[o - 1], s_o.at[o - 1], r_o.at[o - 1], partner).wait_recv()
        out[...] += held[o - 1].astype(F32)
    for copy in sends:
        copy.wait_send()


def scatter(part):
    _, half, rows, wide = part.shape
    return pl.pallas_call(
        functools.partial(scatter_kernel, half),
        out_shape=jax.ShapeDtypeStruct((rows, wide), F32),
        in_specs=[pl.BlockSpec(memory_space=pltpu.VMEM)],
        out_specs=pl.BlockSpec(memory_space=pltpu.VMEM),
        scratch_shapes=[
            pltpu.VMEM((half, rows, wide), BF),
            pltpu.VMEM((half - 1, rows, wide), BF),
            pltpu.VMEM((half - 1, rows, wide), BF),
            pltpu.SemaphoreType.DMA((half,)),
            pltpu.SemaphoreType.DMA((half,)),
            pltpu.SemaphoreType.DMA((half - 1,)),
            pltpu.SemaphoreType.DMA((half - 1,)),
        ],
        compiler_params=pltpu.CompilerParams(collective_id=2, has_side_effects=True),
        name="scatter",
    )(part)


def work_kernel(nb, n, width, hist, states, cot, gain, own, wall, att, gst, part,
                wq, wo, acc, gacc, proj, gproj, ctx, gctx, sems):
    i = pl.program_id(0)
    _, s, dim = states.shape
    rows = nb * s
    lanes = GROUP * 64

    @pl.when(i == 0)
    def _():
        copies = []
        for j in range(n):
            src = own if j == 0 else wall.at[j - 1]
            for k in range(4):
                at = pl.ds(k * width, width)
                dst = wo.at[pl.ds(j * width, width)] if k == 3 else wq.at[pl.ds(k * n * width + j * width, width)]
                copies.append(pltpu.make_async_copy(src.at[at], dst, sems.at[j, k]))
        for copy in copies:
            copy.start()
        acc[...] = jnp.zeros_like(acc)
        gacc[...] = jnp.zeros_like(gacc)
        for copy in copies:
            copy.wait()

    wide = states[...].reshape(rows, dim).astype(F32)
    inv = lax.rsqrt(jnp.mean(wide * wide, axis=-1, keepdims=True) + 1e-06)
    unit = wide * inv
    normed = (unit * gain[...]).astype(BF)
    for k in range(3):
        cols = pl.ds(k * dim, dim)
        proj[:, cols] = dot(normed, wq[cols, :], 1, 1).astype(BF)
    pos = lax.broadcasted_iota(jnp.int32, (s, dim), 0)
    mcot = jnp.concatenate(
        [jnp.where(pos < LEVELS * hist[i * nb + b], cot[b].astype(F32), 0.0) for b in range(nb)], axis=0
    ).astype(BF)
    gctx[...] = dot(mcot, wo[...], 1, 1).astype(BF)

    pack = PACK * 64
    lane = lax.broadcasted_iota(jnp.int32, (s, pack), 1) // 64
    key_pos = lax.broadcasted_iota(jnp.int32, (PACK, s, s), 1)

    only = [(lane == h).astype(F32).astype(BF) for h in range(PACK)]

    def spread(x):
        return jnp.concatenate([x * only[h] for h in range(PACK)], axis=0)

    def fold(x):
        out = x[(PACK - 1) * s :]
        for h in range(PACK - 1):
            out = jnp.where(lane == h, x[h * s : (h + 1) * s], out)
        return out.astype(BF)

    @pl.loop(0, nb, unroll=4)
    def _(b):
        at = pl.ds(pl.multiple_of(b * s, 16), s)
        keep = key_pos < LEVELS * hist[i * nb + b]
        for g in range(dim // pack):
            cols = [pl.ds(k * dim + g * pack, pack) for k in range(3)]
            here = pl.ds(g * pack, pack)
            q, gc = proj[at, cols[0]], gctx[at, here]
            kk, vv = spread(proj[at, cols[1]]), spread(proj[at, cols[2]])
            sc = dot(kk, q, 1, 1).reshape(PACK, s, s)
            sc = jnp.where(keep, sc, -1e30)
            ex = jnp.exp(sc - jnp.max(sc, axis=1, keepdims=True))
            prob = ex * (1.0 / jnp.sum(ex, axis=1, keepdims=True))
            pb = prob.reshape(PACK * s, s).astype(BF)
            ctx[at, here] = dot(pb, vv, 0, 0).astype(BF)
            gp = dot(vv, gc, 1, 1).reshape(PACK, s, s)
            delta = jnp.sum(prob * gp, axis=1, keepdims=True)
            ds = (prob * (gp - delta)).reshape(PACK * s, s).astype(BF)
            gproj[at, cols[0]] = dot(ds, kk, 0, 0).astype(BF)
            gproj[at, cols[1]] = fold(dot(ds, q, 1, 0))
            gproj[at, cols[2]] = fold(dot(pb, gc, 1, 0))

    att[...] = (wide + dot(ctx[...], wo[...], 1, 0)).astype(BF).reshape(nb, s, dim)
    gn = dot(gproj[...], wq[...], 1, 0)
    for k in range(3):
        acc[:, k * lanes : (k + 1) * lanes] += dot(normed, gproj[:, k * dim : k * dim + lanes], 0, 0)
    acc[:, 3 * lanes :] += dot(mcot, ctx[:, :lanes], 0, 0)
    gacc[...] += jnp.sum((gn * unit).reshape(rows // 8, 8, dim), axis=0)
    gu = gn * gain[...]
    corr = jnp.mean(gu * unit, axis=-1, keepdims=True)
    gst[...] = (mcot.astype(F32) + inv * (gu - unit * corr)).astype(BF).reshape(nb, s, dim)

    @pl.when(i == pl.num_programs(0) - 1)
    def _():
        total = jnp.sum(gacc[...], axis=0, keepdims=True)
        column = jnp.broadcast_to(total, (128, dim)).T
        high = column.astype(BF).astype(F32)
        at = lax.broadcasted_iota(jnp.int32, (dim, 128), 1)
        last = slice(4 * lanes - 128, 4 * lanes)
        acc[:, last] = jnp.where(at < 64, acc[:, last], jnp.where(at < 96, high, column - high))
        _, half, piece, _ = part.shape
        for t in range(2 * half):
            part[t % 2, t // 2] = acc[t * piece : (t + 1) * piece, :].astype(BF)


def work(states, hist, gain, own, wall, cot, n, nd):
    count, s, dim = states.shape
    nb = 4 if count % 4 == 0 else 1
    rows, lanes = nb * s, GROUP * 64
    width = dim // n
    block = pl.BlockSpec((nb, s, dim), lambda i, *_: (i, 0, 0))
    piece = (2, nd // 2, dim // nd, 4 * lanes)
    return pl.pallas_call(
        functools.partial(work_kernel, nb, n, width),
        out_shape=(
            jax.ShapeDtypeStruct(states.shape, BF),
            jax.ShapeDtypeStruct(states.shape, BF),
            jax.ShapeDtypeStruct(piece, BF),
        ),
        grid_spec=pltpu.PrefetchScalarGridSpec(
            num_scalar_prefetch=1,
            grid=(count // nb,),
            in_specs=[
                block,
                block,
                pl.BlockSpec((1, dim), lambda i, *_: (0, 0)),
                pl.BlockSpec(memory_space=pl.ANY),
                pl.BlockSpec(memory_space=pl.ANY),
            ],
            out_specs=[block, block, pl.BlockSpec(piece, lambda i, *_: (0, 0, 0, 0))],
            scratch_shapes=[
                pltpu.VMEM((3 * dim, dim), BF),
                pltpu.VMEM((dim, dim), BF),
                pltpu.VMEM((dim, 4 * lanes), F32),
                pltpu.VMEM((8, dim), F32),
                pltpu.VMEM((rows, 3 * dim), BF),
                pltpu.VMEM((rows, 3 * dim), BF),
                pltpu.VMEM((rows, dim), BF),
                pltpu.VMEM((rows, dim), BF),
                pltpu.SemaphoreType.DMA((n, 4)),
            ],
        ),
        compiler_params=pltpu.CompilerParams(
            dimension_semantics=("arbitrary",), vmem_limit_bytes=56 * 1024 * 1024
        ),
        name="work",
    )(hist, states, cot, gain.reshape(1, dim), own, wall)


def body(nd, n, states, hist_len, norm_gain, qkv_weight, output_weight, cotangent):
    dim, _, heads, size = qkv_weight.shape
    width = heads * size
    lanes = GROUP * 64
    own = jnp.concatenate([qkv_weight.reshape(dim, 3 * width).T, output_weight.reshape(width, dim)], axis=0)
    wall = gather(own.reshape(PIECES, 4 * width // PIECES, dim), n).reshape(n - 1, 4 * width, dim)
    attended, grad_states, part = work(states, hist_len, norm_gain, own, wall, cotangent, n, nd)
    summed = scatter(part)
    grads = summed.reshape(dim // nd, 4, lanes)
    grad_qkv = grads[:, :3, :width].reshape(dim // nd, 3, heads, size)
    grad_out = grads[:, 3, :width].T.reshape(heads, size, dim // nd)
    grad_gain = grads[:, 3, 192] + grads[:, 3, 224]
    return attended, grad_states, grad_qkv, grad_out, grad_gain


def solution(mesh):
    placed = (
        P("dp", None, None),
        P("dp"),
        P(),
        P(None, None, "mp", None),
        P("mp", None, None),
        P("dp", None, None),
    )
    return jax.shard_map(
        functools.partial(body, mesh.shape["dp"], mesh.shape["mp"]),
        mesh=mesh,
        in_specs=placed,
        out_specs=(
            P("dp", None, None),
            P("dp", None, None),
            P("dp", None, "mp", None),
            P("mp", None, "dp"),
            P("dp"),
        ),
        check_vma=False,
    )
```
